32 devices in a mesh: swath: 2 (over x), band: 16 (over z, y, core).
Axes of the slice: x: 2, y: 2, z: 4, core: 2. Of those that a mesh axis runs over, the one named last changes fastest.
Arguments:
- design: bfloat16 [512, 16384], P(('swath', 'band')), parts along dimension 0, may hold values from 0 to 1
- row_taps: bfloat16 [8, 33], replicated, may hold values from -1 to 1
- column_taps: bfloat16 [8, 33], replicated, may hold values from -1 to 1
- kernel_weight: float32 [8], replicated, may hold values from 0.5 to 2
- interp: bfloat16 [32, 8], replicated, may hold values from 0 to 0.29882812
- block_shift: int32 [2, 4, 16], P(None, 'swath', 'band'), parts along dimension 1, may hold values from -24 to 24
- block_phase: int32 [2, 4, 16], P(None, 'swath', 'band'), parts along dimension 1, may hold values from 0 to 31
- care: int32 [4, 16], P('swath', 'band'), parts along dimension 0, may hold values 0 or 1
- image: bfloat16 [512, 16384], P('swath', 'band'), parts along dimension 0, may hold values from 0 to 20, as said below
Outputs:
- diff_map: bfloat16 [512, 16384], P('swath', 'band'), parts along dimension 0
The draws below stay inside these ranges and needn't reach their ends.
There are 2 independent parts, one for each index of `swath`. The reference program is written for one: setup_inputs(seed, part) draws one part's arguments, and reference() takes and returns one part's arrays. A program takes and returns all parts, laid end to end along the dimension named above; an argument that names none is the same for every part. Nothing has to cross between parts.
Inputs may be any that keep to these rules, and one draw needn't show every extreme that they name: `image`: nonnegative intensities.
All inputs are finite; a program needn't handle non-finite values. No bound on the sum of `care` on one device may be relied on, other than what follows from the above.
Results may differ from the reference program's by a relative error of at most 0.0045.
Values may be sent and summed in bfloat16 or wider, within the bound.
A program may use at most 64 MiB of HBM per device.

```python
import math
import jax
import jax.numpy as jnp
from jax import lax

W = 16384
NK = 8
KH = 16
SHIFT = 24
IH = 4
NF = 32
BLK = 128
P_SIZE = 28
H = 256
CW = 1024
BROWS = 2
N_BAND = 16


def draw_image(key, part):
    first = jax.random.fold_in(jax.random.fold_in(key, 7), 0)
    columns = jnp.arange(W, dtype=jnp.float32)
    ramp = 1.0 + 2.0 * columns / (W - 1)
    base = jax.random.uniform(first, (H, W), jnp.float32, 0.5, 1.5)
    return (base * ramp[None, :]).astype(jnp.bfloat16)


def with_ends(values, own_key, smallest, high):
    longest = values.shape.index(max(values.shape))
    spots = []
    for shift in (0, 1):
        where = [jax.random.randint(jax.random.fold_in(own_key, axis), (), 0, length) for axis, length in enumerate(values.shape)]
        where[longest] = (where[longest] + shift) % values.shape[longest]
        spots.append(tuple(where))
    return values.at[spots[0]].set(smallest).at[spots[1]].set(high)


def block_scale(rng, dims, shards, low, top_value):
    def one(dim, blocks):
        heights = jax.random.uniform(jax.random.fold_in(jax.random.fold_in(rng, 6), dim), (blocks,), jnp.float32, low / len(shards), top_value / len(shards))
        return jnp.repeat(jnp.exp(heights), dims[dim] // blocks).reshape((-1,) + (1,) * (len(dims) - dim - 1))

    level = one(*shards[0])
    for cut in shards[1:]:
        level = level * one(*cut)
    return level


def normal_values(rng, extent, width, bound, held_as=jnp.bfloat16):
    values = jax.random.normal(rng, extent, jnp.float32) * width
    return jnp.minimum(jnp.maximum(values, -bound), bound).astype(held_as)


def setup_inputs(seed: int = 0, part: int = 0) -> dict:
    arg_keys = jax.random.split(jax.random.key(seed), 10)
    part_splits = jax.random.split(jax.random.fold_in(arg_keys[9], part), 10)
    design = jnp.clip(1.0 * jax.random.uniform(part_splits[0], (H, W), jnp.float32) ** block_scale(part_splits[0], (H, W), ((0, 16),), -0.2, 0.2), 0.0, 1.0).astype(jnp.bfloat16)
    row_taps = normal_values(arg_keys[1], (NK, 2 * KH + 1), (2 * KH + 1) ** -0.5, 1.0)
    column_taps = normal_values(arg_keys[2], (NK, 2 * KH + 1), (2 * KH + 1) ** -0.5, 1.0)
    kernel_weight = jnp.clip(jnp.exp(jax.random.uniform(arg_keys[3], (NK,), jnp.float32, math.log(0.5), math.log(2.0))), 0.5, 2.0)
    interp = jnp.clip(jax.random.uniform(arg_keys[4], (NF, 2 * IH), jnp.float32, 0.0, 0.29882812), 0.0, 0.29882812).astype(jnp.bfloat16)
    block_shift = with_ends(jax.random.randint(part_splits[5], (2, BROWS, N_BAND), -SHIFT, SHIFT + 1), jax.random.fold_in(part_splits[5], 1), -SHIFT, SHIFT).astype(jnp.int32)
    block_phase = with_ends(jax.random.randint(part_splits[6], (2, BROWS, N_BAND), 0, NF), jax.random.fold_in(part_splits[6], 1), 0, NF - 1).astype(jnp.int32)
    care = with_ends((jax.random.randint(part_splits[7], (BROWS, N_BAND), 0, 3) < 2).astype(jnp.int32), jax.random.fold_in(part_splits[7], 1), 0, 1)
    image = draw_image(jax.random.fold_in(jax.random.fold_in(arg_keys[9], part), 71), part)
    return {"design": design, "row_taps": row_taps, "column_taps": column_taps, "kernel_weight": kernel_weight, "interp": interp, "block_shift": block_shift, "block_phase": block_phase, "care": care, "image": image}


epsilon = 1e-05

def band_matrix(offsets, phases, interp, size_out, size_in):
    table = jax.nn.one_hot(phases, NF, dtype=jnp.float32)
    weights = jnp.dot(table, interp.astype(jnp.float32), precision=lax.Precision.HIGHEST)
    outer = jnp.arange(size_out, dtype=jnp.int32)
    inner = jnp.arange(size_in, dtype=jnp.int32)
    position = inner[None, None, :] - outer[None, :, None] - offsets[:, None, None] + (IH - 1 - P_SIZE)
    matrix = jnp.zeros(position.shape, jnp.float32)
    for tap in range(2 * IH):
        matrix = matrix + jnp.where(position == tap, weights[:, tap][:, None, None], 0.0)
    return matrix.astype(jnp.bfloat16)

def warp_strip(framed, shifts, phases, interp):
    height = framed.shape[0] - BLK - 2 * P_SIZE
    across = framed.shape[1]
    strip_cols = across - 2 * P_SIZE
    count = height // BLK
    upper = framed[:height].reshape(count, BLK, across)[:, :P_SIZE]
    middle = framed[P_SIZE:P_SIZE + height].reshape(count, BLK, across)
    lower = framed[BLK + P_SIZE:BLK + P_SIZE + height].reshape(count, BLK, across)[:, :P_SIZE]
    blocks = jnp.concatenate([upper, middle, lower], axis=1)
    row_matrix = band_matrix(shifts[0], phases[0], interp, BLK, BLK + 2 * P_SIZE)
    column_matrix = band_matrix(shifts[1], phases[1], interp, strip_cols, across)
    partial_value = jnp.einsum('brs,bsc->brc', row_matrix.astype(jnp.float32), blocks.astype(jnp.float32), precision=lax.Precision.HIGHEST).astype(jnp.bfloat16)
    return jnp.einsum('brs,bcs->brc', partial_value.astype(jnp.float32), column_matrix.astype(jnp.float32), precision=lax.Precision.HIGHEST)

def finish(warped, strip, cares):
    count, rows, cols = warped.shape
    measured = strip.reshape(count, rows, cols).astype(jnp.float32)
    difference = (cares.astype(jnp.float32)[:, None, None] * (measured - warped)).reshape(count * rows, cols)
    padded = jnp.pad(difference, ((1, 1), (0, 0)))
    return difference + 0.5 * (padded[:-2] + padded[2:])

def reference(design, row_taps, column_taps, kernel_weight, interp, block_shift, block_phase, care, image):
    plane = design.astype(jnp.float32)[None, None]

    def add_kernel(kernel, total):
        row_filter = row_taps[kernel].astype(jnp.float32).reshape(1, 1, 2 * KH + 1, 1)
        smoothed = lax.conv_general_dilated(plane, row_filter, (1, 1), ((KH, KH), (0, 0)), precision=lax.Precision.HIGHEST).astype(jnp.bfloat16)
        column_filter = column_taps[kernel].astype(jnp.float32).reshape(1, 1, 1, 2 * KH + 1)
        field = lax.conv_general_dilated(smoothed.astype(jnp.float32), column_filter, (1, 1), ((0, 0), (KH, KH)), precision=lax.Precision.HIGHEST)[0, 0]
        return total + kernel_weight[kernel] * field * field
    total = lax.fori_loop(0, NK, add_kernel, jnp.zeros((H, W), jnp.float32))
    intensity = total.astype(jnp.bfloat16)
    padded = jnp.pad(intensity, ((P_SIZE, BLK + P_SIZE), (P_SIZE, P_SIZE)))
    strips = image.reshape(H, N_BAND, CW).transpose(1, 0, 2)
    starts = (jnp.arange(N_BAND, dtype=jnp.int32) * CW).astype(jnp.int32)

    def one_strip(items):
        start, shifts, phases, cares, strip = items
        framed = lax.dynamic_slice_in_dim(padded, start, CW + 2 * P_SIZE, axis=1)
        warped = warp_strip(framed, shifts, phases, interp)
        return finish(warped, strip, cares)
    filtered = lax.map(one_strip, (starts, jnp.moveaxis(block_shift, 2, 0), jnp.moveaxis(block_phase, 2, 0), care.T, strips))
    cells = H * W
    mean = jnp.sum(filtered) / cells
    variance = jnp.sum((filtered - mean) * (filtered - mean)) / cells
    care_rows = jnp.repeat(care.T.astype(jnp.float32), BLK, axis=1)
    result = care_rows[:, :, None] * (filtered - mean) * lax.rsqrt(variance + epsilon)
    return result.transpose(1, 0, 2).reshape(H, W).astype(jnp.bfloat16)
```

```python
import functools

import jax
import jax.numpy as jnp
from jax import lax
from jax.experimental import pallas as pl
from jax.experimental.pallas import tpu as pltpu
from jax.sharding import PartitionSpec as P

NK = 8
KH = 16
IH = 4
BLK = 128
P_SIZE = 28
LANES = 128
EDGE = 32
GROUP = 4
REACH = 2 * KH + 1

epsilon = 1e-05
F32 = jnp.float32
BF16 = jnp.bfloat16


def banded(offset, taps, shape):
    place = (
        lax.broadcasted_iota(jnp.int32, shape, 0)
        - lax.broadcasted_iota(jnp.int32, shape, 1)
        - offset
    )
    matrix = jnp.zeros(shape, F32)
    for tap in range(taps.shape[1]):
        matrix = jnp.where(place == tap, taps[:, tap : tap + 1], matrix)
    return matrix


def banded_rows(offset, taps, shape):
    place = (
        lax.broadcasted_iota(jnp.int32, shape, 1)
        - lax.broadcasted_iota(jnp.int32, shape, 0)
        - offset
    )
    matrix = jnp.zeros(shape, F32)
    for tap in range(taps.shape[1]):
        matrix = jnp.where(place == tap, taps[:, tap : tap + 1], matrix)
    return matrix


def kernel(
    n, height, width,
    weight_ref, shift_ref, phase_ref, care_ref,
    design_ref, row_ref, column_ref, interp_ref, image_hbm,
    out_ref,
    sendbuf, recv, image, row_mats, column_mats, taps, table, smooth, intensity,
    diff, filt, stats_mine, stats_all,
    send_sem, recv_sem, stat_send, stat_recv, image_sem,
):
    me = lax.axis_index("band")
    rows = design_ref.shape[0]
    strip = width // n
    panels = strip // LANES
    wide = strip + LANES
    block_rows = GROUP * rows
    window = block_rows + 2 * KH
    steps = n // GROUP

    barrier = pltpu.get_barrier_semaphore()

    def greet(i, carry):
        peer = lax.rem(me + i, n)
        pl.semaphore_signal(
            barrier, inc=1, device_id={"band": peer}, device_id_type=pl.DeviceIdType.MESH
        )
        return carry

    lax.fori_loop(1, n, greet, 0)

    fetch = pltpu.make_async_copy(image_hbm, image, image_sem)
    fetch.start()

    lane = lax.broadcasted_iota(jnp.int32, (rows, LANES), 1)
    low = lane < LANES // 2
    zero_panel = jnp.zeros((rows, LANES), BF16)
    for owner in range(n):
        start = owner * strip
        sendbuf[owner, :, :strip] = design_ref[:, start : start + strip]
        after = design_ref[:, start + strip : start + strip + LANES] if owner < n - 1 else zero_panel
        before = design_ref[:, start - LANES : start] if owner > 0 else zero_panel
        sendbuf[owner, :, strip:] = jnp.where(low, after, before)

    pl.semaphore_wait(barrier, n - 1)

    def copy_to(peer):
        return pltpu.make_async_remote_copy(
            src_ref=sendbuf.at[peer],
            dst_ref=recv.at[pl.ds(pl.multiple_of(KH + me * rows, rows), rows), :],
            send_sem=send_sem.at[peer],
            recv_sem=recv_sem.at[me],
            device_id={"band": peer},
            device_id_type=pl.DeviceIdType.MESH,
        )

    def copy_from(peer):
        return pltpu.make_async_remote_copy(
            src_ref=sendbuf.at[peer],
            dst_ref=recv.at[pl.ds(pl.multiple_of(KH + peer * rows, rows), rows), :],
            send_sem=send_sem.at[peer],
            recv_sem=recv_sem.at[peer],
            device_id={"band": peer},
            device_id_type=pl.DeviceIdType.MESH,
        )

    def send(i, carry):
        peer = lax.rem(me + n // 2 + i, n)

        @pl.when(peer != me)
        def _():
            copy_to(peer).start()

        return carry

    lax.fori_loop(0, n, send, 0)

    recv[pl.ds(pl.multiple_of(KH + me * rows, rows), rows), :] = sendbuf[me]
    recv[:KH, :] = jnp.zeros((KH, wide), BF16)
    recv[KH + height :, :] = jnp.zeros((KH, wide), BF16)
    intensity[:EDGE, :] = jnp.zeros((EDGE, wide), BF16)
    intensity[EDGE + height :, :] = jnp.zeros((EDGE, wide), BF16)
    diff[:8, :] = jnp.zeros((8, strip), F32)
    diff[8 + height :, :] = jnp.zeros((8, strip), F32)

    taps[:NK, :REACH] = row_ref[...].astype(F32)
    taps[NK:, :REACH] = column_ref[...].astype(F32)
    table[:, : 2 * IH] = interp_ref[...].astype(F32)

    def build(k, carry):
        row_taps = taps[pl.ds(k, 1), :REACH]
        row_mats[pl.ds(pl.multiple_of(k * block_rows, block_rows), block_rows), :] = banded_rows(
            0, row_taps, (block_rows, window)
        ).astype(BF16)
        column_taps = taps[pl.ds(NK + k, 1), :REACH]
        column_mats[k] = banded(LANES - P_SIZE - KH, column_taps, (2 * LANES, LANES)).astype(BF16)
        return carry

    lax.fori_loop(0, NK, build, 0)

    rising = me < n // 2

    def arrived(place):
        band = jnp.where(rising, place, n - 1 - place)

        @pl.when(jnp.logical_and(place < n, band != me))
        def _():
            copy_from(band).wait_recv()

    first_column = me * strip - P_SIZE
    column = lax.broadcasted_iota(jnp.int32, (block_rows, LANES), 1)

    arrived(jnp.int32(0))

    def render(i, carry):
        for more in range(1, GROUP + 1):
            arrived(i * GROUP + more)
        group = jnp.where(rising, i, steps - 1 - i)
        start = pl.multiple_of(group * block_rows, block_rows)
        smooth[...] = jnp.dot(
            row_mats[...], recv[pl.ds(start, window), :], preferred_element_type=F32
        ).astype(BF16)
        total = jnp.zeros(((panels + 1) * block_rows, LANES), F32)
        for k in range(NK):
            own = smooth[k * block_rows : (k + 1) * block_rows, :]
            pieces = [jnp.concatenate([own[:, strip:], own[:, :LANES]], axis=1)]
            pieces += [own[:, (p - 1) * LANES : (p + 1) * LANES] for p in range(1, panels + 1)]
            field = jnp.dot(
                jnp.concatenate(pieces, axis=0), column_mats[k], preferred_element_type=F32
            )
            total = total + weight_ref[k] * field * field
        into = pl.multiple_of(EDGE + start, EDGE)
        for p in range(panels + 1):
            part = total[p * block_rows : (p + 1) * block_rows]
            if p in (0, panels):
                at = column + (first_column + p * LANES)
                part = jnp.where(jnp.logical_and(at >= 0, at < width), part, 0.0)
            intensity[pl.ds(into, block_rows), p * LANES : (p + 1) * LANES] = part.astype(BF16)
        return carry

    lax.fori_loop(0, steps, render, 0)

    fetch.wait()

    def warp(b, carry):
        u = table[pl.ds(phase_ref[0, b, 0], 1), : 2 * IH]
        v = table[pl.ds(phase_ref[1, b, 0], 1), : 2 * IH]
        row_matrix = banded_rows(
            EDGE + 1 - IH + shift_ref[0, b, 0], u, (BLK, BLK + 2 * EDGE)
        ).astype(BF16)
        column_matrix = banded(
            P_SIZE + 1 - IH + shift_ref[1, b, 0], v, (2 * LANES, LANES)
        ).astype(BF16)
        start = pl.multiple_of(b * BLK, BLK)
        partial = jnp.dot(
            row_matrix, intensity[pl.ds(start, BLK + 2 * EDGE), :], preferred_element_type=F32
        ).astype(BF16)
        pieces = [partial[:, p * LANES : (p + 2) * LANES] for p in range(panels)]
        warped = jnp.dot(
            jnp.concatenate(pieces, axis=0), column_matrix, preferred_element_type=F32
        )
        care = care_ref[b, 0].astype(F32)
        for p in range(panels):
            measured = image[pl.ds(start, BLK), p * LANES : (p + 1) * LANES].astype(F32)
            diff[pl.ds(pl.multiple_of(8 + start, 8), BLK), p * LANES : (p + 1) * LANES] = care * (
                measured - warped[p * BLK : (p + 1) * BLK]
            )
        return carry

    lax.fori_loop(0, height // BLK, warp, 0)

    part_rows = 32

    def stencil(i, carry):
        first, second = carry
        start = pl.multiple_of(i * part_rows, part_rows)
        around = diff[pl.ds(start, part_rows + 16), :]
        middle = around[8 : 8 + part_rows]
        value = middle + 0.5 * (around[7 : 7 + part_rows] + around[9 : 9 + part_rows])
        filt[pl.ds(start, part_rows), :] = value
        square = value * value
        for r in range(0, part_rows, 8):
            for p in range(panels):
                first = first + value[r : r + 8, p * LANES : (p + 1) * LANES]
                second = second + square[r : r + 8, p * LANES : (p + 1) * LANES]
        return first, second

    none = jnp.zeros((8, LANES), F32)
    first, second = lax.fori_loop(0, height // part_rows, stencil, (none, none))
    stats_mine[:8, :] = first
    stats_mine[8:, :] = second

    def stat_to(peer):
        return pltpu.make_async_remote_copy(
            src_ref=stats_mine,
            dst_ref=stats_all.at[me],
            send_sem=stat_send.at[peer],
            recv_sem=stat_recv.at[me],
            device_id={"band": peer},
            device_id_type=pl.DeviceIdType.MESH,
        )

    def stat_from(peer):
        return pltpu.make_async_remote_copy(
            src_ref=stats_mine,
            dst_ref=stats_all.at[peer],
            send_sem=stat_send.at[peer],
            recv_sem=stat_recv.at[peer],
            device_id={"band": peer},
            device_id_type=pl.DeviceIdType.MESH,
        )

    def send_stats(i, carry):
        peer = lax.rem(me + n // 2 + i, n)

        @pl.when(peer != me)
        def _():
            stat_to(peer).start()

        return carry

    lax.fori_loop(0, n, send_stats, 0)
    stats_all[me] = stats_mine[...]

    def finish_sends(i, carry):
        peer = lax.rem(me + i, n)
        copy_to(peer).wait_send()
        return carry

    lax.fori_loop(1, n, finish_sends, 0)

    def take_stats(i, carry):
        peer = lax.rem(me + i, n)
        stat_from(peer).wait_recv()
        stat_to(peer).wait_send()
        return carry

    lax.fori_loop(1, n, take_stats, 0)

    sums = lax.fori_loop(
        0, n, lambda i, carry: carry + stats_all[i], jnp.zeros((16, LANES), F32)
    )
    cells = height * width
    mean = jnp.sum(jnp.sum(sums[:8], axis=1, keepdims=True), axis=0, keepdims=True) / cells
    power = jnp.sum(jnp.sum(sums[8:], axis=1, keepdims=True), axis=0, keepdims=True) / cells
    scale = lax.rsqrt(power - mean * mean + epsilon)

    per_block = BLK // part_rows

    def normalize(i, carry):
        start = pl.multiple_of(i * part_rows, part_rows)
        care = care_ref[i // per_block, 0].astype(F32)
        value = filt[pl.ds(start, part_rows), :]
        out_ref[pl.ds(start, part_rows), :] = (care * ((value - mean) * scale)).astype(BF16)
        return carry

    lax.fori_loop(0, height // part_rows, normalize, 0)


def on_device(
    design, row_taps, column_taps, kernel_weight, interp, block_shift, block_phase, care, image
):
    n = lax.axis_size("band")
    rows, width = design.shape
    height, strip = image.shape
    wide = strip + LANES
    block_rows = GROUP * rows
    window = block_rows + 2 * KH
    smem = pl.BlockSpec(memory_space=pltpu.SMEM)
    vmem = pl.BlockSpec(memory_space=pltpu.VMEM)
    return pl.pallas_call(
        functools.partial(kernel, n, height, width),
        out_shape=jax.ShapeDtypeStruct((height, strip), BF16),
        in_specs=[smem] * 4 + [vmem] * 4 + [pl.BlockSpec(memory_space=pl.ANY)],
        out_specs=vmem,
        scratch_shapes=[
            pltpu.VMEM((n, rows, wide), BF16),
            pltpu.VMEM((height + 2 * KH, wide), BF16),
            pltpu.VMEM((height, strip), BF16),
            pltpu.VMEM((NK * block_rows, window), BF16),
            pltpu.VMEM((NK, 2 * LANES, LANES), BF16),
            pltpu.VMEM((2 * NK, LANES), F32),
            pltpu.VMEM((interp.shape[0], LANES), F32),
            pltpu.VMEM((NK * block_rows, wide), BF16),
            pltpu.VMEM((height + 2 * EDGE, wide), BF16),
            pltpu.VMEM((height + 16, strip), F32),
            pltpu.VMEM((height, strip), F32),
            pltpu.VMEM((16, LANES), F32),
            pltpu.VMEM((n, 16, LANES), F32),
            pltpu.SemaphoreType.DMA((n,)),
            pltpu.SemaphoreType.DMA((n,)),
            pltpu.SemaphoreType.DMA((n,)),
            pltpu.SemaphoreType.DMA((n,)),
            pltpu.SemaphoreType.DMA,
        ],
        compiler_params=pltpu.CompilerParams(collective_id=0, has_side_effects=True),
    )(
        kernel_weight, block_shift, block_phase, care,
        design, row_taps, column_taps, interp, image,
    )


def solution(mesh):
    placed = (
        P(("swath", "band"), None),
        P(),
        P(),
        P(),
        P(),
        P(None, "swath", "band"),
        P(None, "swath", "band"),
        P("swath", "band"),
        P("swath", "band"),
    )
    return jax.shard_map(
        on_device, mesh=mesh, in_specs=placed, out_specs=P("swath", "band"), check_vma=False
    )
```

```python
import functools

import jax
import jax.numpy as jnp
from jax import lax
from jax.experimental import pallas as pl
from jax.experimental.pallas import tpu as pltpu
from jax.sharding import PartitionSpec as P

NK = 8
KH = 16
IH = 4
BLK = 128
P_SIZE = 28
LANES = 128
EDGE = 32
PART = 32
GROUP = 4
REACH = 2 * KH + 1

epsilon = 1e-05
F32 = jnp.float32
BF16 = jnp.bfloat16


def banded(offset, taps, shape):
    place = (
        lax.broadcasted_iota(jnp.int32, shape, 0)
        - lax.broadcasted_iota(jnp.int32, shape, 1)
        - offset
    )
    matrix = jnp.zeros(shape, F32)
    for tap, value in enumerate(taps):
        matrix = jnp.where(place == tap, value, matrix)
    return matrix


def banded_rows(offset, taps, shape):
    place = (
        lax.broadcasted_iota(jnp.int32, shape, 1)
        - lax.broadcasted_iota(jnp.int32, shape, 0)
        - offset
    )
    matrix = jnp.zeros(shape, F32)
    for tap, value in enumerate(taps):
        matrix = jnp.where(place == tap, value, matrix)
    return matrix


def kernel(
    n, height, width,
    weight_hbm, shift_hbm, phase_hbm, care_hbm,
    design_hbm, row_hbm, column_hbm, interp_hbm, image_hbm,
    filt_hbm, mean_ref, scale_ref,
    weight_ref, shift_ref, phase_ref, care_ref,
    design_ref, row_ref, column_ref, interp_ref,
    sendbuf, recv, image, row_mats, column_mats, taps, table, smooth, intensity,
    diff, filt, stats_mine, stats_all,
    send_sem, recv_sem, stat_send, stat_recv, load_sem, store_sem,
):
    me = lax.axis_index("band")
    rows = design_ref.shape[0]
    strip = width // n
    panels = strip // LANES
    wide = strip + LANES
    block_rows = GROUP * rows
    window = block_rows + 2 * KH
    steps = n // GROUP

    barrier = pltpu.get_barrier_semaphore()

    def greet(i, carry):
        peer = lax.rem(me + i, n)
        pl.semaphore_signal(
            barrier, inc=1, device_id={"band": peer}, device_id_type=pl.DeviceIdType.MESH
        )
        return carry

    lax.fori_loop(1, n, greet, 0)

    loads = [
        pltpu.make_async_copy(source, target, load_sem.at[i])
        for i, (source, target) in enumerate(
            [
                (design_hbm, design_ref),
                (row_hbm, row_ref),
                (column_hbm, column_ref),
                (interp_hbm, interp_ref),
                (weight_hbm, weight_ref),
                (shift_hbm, shift_ref),
                (phase_hbm, phase_ref),
                (care_hbm, care_ref),
                (image_hbm, image),
            ]
        )
    ]
    for load in loads:
        load.start()
    loads[0].wait()

    lane = lax.broadcasted_iota(jnp.int32, (rows, LANES), 1)
    low = lane < LANES // 2
    zero_panel = jnp.zeros((rows, LANES), BF16)
    for owner in range(n):
        start = owner * strip
        sendbuf[owner, :, :strip] = design_ref[:, start : start + strip]
        after = design_ref[:, start + strip : start + strip + LANES] if owner < n - 1 else zero_panel
        before = design_ref[:, start - LANES : start] if owner > 0 else zero_panel
        sendbuf[owner, :, strip:] = jnp.where(low, after, before)

    pl.semaphore_wait(barrier, n - 1)

    def copy_to(peer):
        return pltpu.make_async_remote_copy(
            src_ref=sendbuf.at[peer],
            dst_ref=recv.at[pl.ds(pl.multiple_of(KH + me * rows, rows), rows), :],
            send_sem=send_sem.at[peer],
            recv_sem=recv_sem.at[me],
            device_id={"band": peer},
            device_id_type=pl.DeviceIdType.MESH,
        )

    def copy_from(peer):
        return pltpu.make_async_remote_copy(
            src_ref=sendbuf.at[peer],
            dst_ref=recv.at[pl.ds(pl.multiple_of(KH + peer * rows, rows), rows), :],
            send_sem=send_sem.at[peer],
            recv_sem=recv_sem.at[peer],
            device_id={"band": peer},
            device_id_type=pl.DeviceIdType.MESH,
        )

    def send(i, carry):
        @pl.when(me + i < n)
        def _():
            copy_to(me + i).start()

        @pl.when(me - i >= 0)
        def _():
            copy_to(me - i).start()

        return carry

    lax.fori_loop(1, n, send, 0)

    recv[pl.ds(pl.multiple_of(KH + me * rows, rows), rows), :] = sendbuf[me]
    recv[:KH, :] = jnp.zeros((KH, wide), BF16)
    recv[KH + height :, :] = jnp.zeros((KH, wide), BF16)
    intensity[:EDGE, :] = jnp.zeros((EDGE, wide), BF16)
    intensity[EDGE + height :, :] = jnp.zeros((EDGE, wide), BF16)
    diff[:8, :] = jnp.zeros((8, strip), F32)
    diff[8 + height :, :] = jnp.zeros((8, strip), F32)

    for load in loads[1:-1]:
        load.wait()
    taps[:NK, :REACH] = row_ref[...].astype(F32)
    taps[NK:, :REACH] = column_ref[...].astype(F32)
    table[...] = interp_ref[...].astype(F32)
    phases = lax.broadcasted_iota(jnp.int32, table.shape, 1)

    def chosen(phase):
        row = jnp.sum(jnp.where(phases == phase, table[...], 0.0), axis=1, keepdims=True)
        return [row[t : t + 1] for t in range(2 * IH)]

    def build(k, carry):
        row_taps = [taps[pl.ds(k, 1), t : t + 1] for t in range(REACH)]
        row_mats[pl.ds(pl.multiple_of(k * block_rows, block_rows), block_rows), :] = banded_rows(
            0, row_taps, (block_rows, window)
        ).astype(BF16)
        column_taps = [taps[pl.ds(NK + k, 1), t : t + 1] for t in range(REACH)]
        column_mats[k] = banded(LANES - P_SIZE - KH, column_taps, (2 * LANES, LANES)).astype(BF16)
        return carry

    lax.fori_loop(0, NK, build, 0)

    rising = me < n // 2

    def arrived(place):
        band = jnp.where(rising, place, n - 1 - place)

        @pl.when(jnp.logical_and(place < n, band != me))
        def _():
            copy_from(band).wait_recv()

    first_column = me * strip - P_SIZE
    column = lax.broadcasted_iota(jnp.int32, (block_rows, LANES), 1)

    per_block = BLK // block_rows
    count = height // BLK
    part_rows = PART
    parts = BLK // part_rows

    def render(i, carry):
        for more in range(1, GROUP + 1):
            arrived(i * GROUP + more)
        group = jnp.where(rising, i, steps - 1 - i)
        start = pl.multiple_of(group * block_rows, block_rows)
        smooth[...] = jnp.dot(
            row_mats[...], recv[pl.ds(start, window), :], preferred_element_type=F32
        ).astype(BF16)
        total = jnp.zeros(((panels + 1) * block_rows, LANES), F32)
        for k in range(NK):
            own = smooth[k * block_rows : (k + 1) * block_rows, :]
            pieces = [jnp.concatenate([own[:, strip:], own[:, :LANES]], axis=1)]
            pieces += [own[:, (p - 1) * LANES : (p + 1) * LANES] for p in range(1, panels + 1)]
            field = jnp.dot(
                jnp.concatenate(pieces, axis=0), column_mats[k], preferred_element_type=F32
            )
            total = total + weight_ref[k] * field * field
        into = pl.multiple_of(EDGE + start, EDGE)
        for p in range(panels + 1):
            part = total[p * block_rows : (p + 1) * block_rows]
            if p in (0, panels):
                at = column + (first_column + p * LANES)
                part = jnp.where(jnp.logical_and(at >= 0, at < width), part, 0.0)
            intensity[pl.ds(into, block_rows), p * LANES : (p + 1) * LANES] = part.astype(BF16)

        @pl.when(jnp.logical_and(i >= per_block, lax.rem(i, per_block) == 0))
        def _():
            warp(i // per_block - 1)

        return carry

    def warp(place):
        b = jnp.where(rising, place, count - 1 - place)
        u = chosen(phase_ref[0, 0, b])
        v = chosen(phase_ref[1, 0, b])
        row_matrix = banded_rows(
            EDGE + 1 - IH + shift_ref[0, 0, b], u, (BLK, BLK + 2 * EDGE)
        ).astype(BF16)
        column_matrix = banded(
            P_SIZE + 1 - IH + shift_ref[1, 0, b], v, (2 * LANES, LANES)
        ).astype(BF16)
        start = pl.multiple_of(b * BLK, BLK)
        partial = jnp.dot(
            row_matrix, intensity[pl.ds(start, BLK + 2 * EDGE), :], preferred_element_type=F32
        ).astype(BF16)
        pieces = [partial[:, p * LANES : (p + 2) * LANES] for p in range(panels)]
        warped = jnp.dot(
            jnp.concatenate(pieces, axis=0), column_matrix, preferred_element_type=F32
        )
        care = care_ref[0, b].astype(F32)
        for p in range(panels):
            measured = image[pl.ds(start, BLK), p * LANES : (p + 1) * LANES].astype(F32)
            diff[pl.ds(pl.multiple_of(8 + start, 8), BLK), p * LANES : (p + 1) * LANES] = care * (
                measured - warped[p * BLK : (p + 1) * BLK]
            )

        first_part = place * parts - jnp.where(place > 0, 1, 0)
        last_part = (place + 1) * parts - jnp.where(place < count - 1, 1, 0)
        lax.fori_loop(first_part, last_part, stencil, 0)

    def store(part):
        where = pl.ds(pl.multiple_of(part * part_rows, part_rows), part_rows)
        return pltpu.make_async_copy(filt.at[where], filt_hbm.at[where], store_sem.at[part])

    def stencil(place, carry):
        part = jnp.where(rising, place, count * parts - 1 - place)
        start = pl.multiple_of(part * part_rows, part_rows)
        around = diff[pl.ds(start, part_rows + 16), :]
        middle = around[8 : 8 + part_rows]
        value = middle + 0.5 * (around[7 : 7 + part_rows] + around[9 : 9 + part_rows])
        filt[pl.ds(start, part_rows), :] = value
        store(part).start()
        square = value * value
        first = stats_mine[:8, :]
        second = stats_mine[8:, :]
        for r in range(0, part_rows, 8):
            for p in range(panels):
                first = first + value[r : r + 8, p * LANES : (p + 1) * LANES]
                second = second + square[r : r + 8, p * LANES : (p + 1) * LANES]
        stats_mine[:8, :] = first
        stats_mine[8:, :] = second
        return carry

    loads[-1].wait()
    stats_mine[...] = jnp.zeros((16, LANES), F32)
    arrived(jnp.int32(0))
    lax.fori_loop(0, steps, render, 0)
    warp(jnp.int32(count - 1))

    def stat_to(peer):
        return pltpu.make_async_remote_copy(
            src_ref=stats_mine,
            dst_ref=stats_all.at[me],
            send_sem=stat_send.at[peer],
            recv_sem=stat_recv.at[me],
            device_id={"band": peer},
            device_id_type=pl.DeviceIdType.MESH,
        )

    def stat_from(peer):
        return pltpu.make_async_remote_copy(
            src_ref=stats_mine,
            dst_ref=stats_all.at[peer],
            send_sem=stat_send.at[peer],
            recv_sem=stat_recv.at[peer],
            device_id={"band": peer},
            device_id_type=pl.DeviceIdType.MESH,
        )

    def send_stats(i, carry):
        peer = lax.rem(me + n // 2 + i, n)

        @pl.when(peer != me)
        def _():
            stat_to(peer).start()

        return carry

    lax.fori_loop(0, n, send_stats, 0)
    stats_all[me] = stats_mine[...]

    def finish_sends(i, carry):
        peer = lax.rem(me + i, n)
        copy_to(peer).wait_send()
        return carry

    lax.fori_loop(1, n, finish_sends, 0)

    def take_stats(i, carry):
        peer = lax.rem(me + i, n)
        stat_from(peer).wait_recv()
        stat_to(peer).wait_send()
        return carry

    lax.fori_loop(1, n, take_stats, 0)

    sums = lax.fori_loop(
        0, n, lambda i, carry: carry + stats_all[i], jnp.zeros((16, LANES), F32)
    )
    cells = height * width
    mean = jnp.sum(jnp.sum(sums[:8], axis=1, keepdims=True), axis=0, keepdims=True) / cells
    power = jnp.sum(jnp.sum(sums[8:], axis=1, keepdims=True), axis=0, keepdims=True) / cells
    scale = lax.rsqrt(power - mean * mean + epsilon)
    mean_ref[...] = jnp.broadcast_to(mean, (1, strip))
    for b in range(count):
        scale_ref[b : b + 1, :] = jnp.broadcast_to(care_ref[0, b].astype(F32) * scale, (1, strip))

    def finish_store(part, carry):
        store(part).wait()
        return carry

    lax.fori_loop(0, count * parts, finish_store, 0)


def on_device(
    design, row_taps, column_taps, kernel_weight, interp, block_shift, block_phase, care, image
):
    n = lax.axis_size("band")
    rows, width = design.shape
    height, strip = image.shape
    wide = strip + LANES
    block_rows = GROUP * rows
    window = block_rows + 2 * KH
    count = height // BLK
    hbm = pl.BlockSpec(memory_space=pltpu.HBM)
    vmem = pl.BlockSpec(memory_space=pltpu.VMEM)
    filtered, mean, scale = pl.pallas_call(
        functools.partial(kernel, n, height, width),
        out_shape=(
            jax.ShapeDtypeStruct((height, strip), F32),
            jax.ShapeDtypeStruct((1, strip), F32),
            jax.ShapeDtypeStruct((count, strip), F32),
        ),
        in_specs=[hbm] * 9,
        out_specs=(hbm, vmem, vmem),
        scratch_shapes=[
            pltpu.SMEM((NK,), F32),
            pltpu.SMEM((2, 1, count), jnp.int32),
            pltpu.SMEM((2, 1, count), jnp.int32),
            pltpu.SMEM((1, count), jnp.int32),
            pltpu.VMEM((rows, width), BF16),
            pltpu.VMEM(row_taps.shape, BF16),
            pltpu.VMEM(column_taps.shape, BF16),
            pltpu.VMEM(interp.shape[::-1], BF16),
            pltpu.VMEM((n, rows, wide), BF16),
            pltpu.VMEM((height + 2 * KH, wide), BF16),
            pltpu.VMEM((height, strip), BF16),
            pltpu.VMEM((NK * block_rows, window), BF16),
            pltpu.VMEM((NK, 2 * LANES, LANES), BF16),
            pltpu.VMEM((2 * NK, LANES), F32),
            pltpu.VMEM(interp.shape[::-1], F32),
            pltpu.VMEM((NK * block_rows, wide), BF16),
            pltpu.VMEM((height + 2 * EDGE, wide), BF16),
            pltpu.VMEM((height + 16, strip), F32),
            pltpu.VMEM((height, strip), F32),
            pltpu.VMEM((16, LANES), F32),
            pltpu.VMEM((n, 16, LANES), F32),
            pltpu.SemaphoreType.DMA((n,)),
            pltpu.SemaphoreType.DMA((n,)),
            pltpu.SemaphoreType.DMA((n,)),
            pltpu.SemaphoreType.DMA((n,)),
            pltpu.SemaphoreType.DMA((9,)),
            pltpu.SemaphoreType.DMA((height // PART,)),
        ],
        compiler_params=pltpu.CompilerParams(collective_id=0, has_side_effects=True),
    )(
        kernel_weight,
        jnp.transpose(block_shift, (0, 2, 1)),
        jnp.transpose(block_phase, (0, 2, 1)),
        care.T,
        design,
        row_taps,
        column_taps,
        interp.T,
        image,
    )
    blocks = filtered.reshape(count, BLK, strip)
    out = (blocks - mean[:, None]) * scale[:, None]
    return out.reshape(height, strip).astype(BF16)


def solution(mesh):
    placed = (
        P(("swath", "band"), None),
        P(),
        P(),
        P(),
        P(),
        P(None, "swath", "band"),
        P(None, "swath", "band"),
        P("swath", "band"),
        P("swath", "band"),
    )
    return jax.shard_map(
        on_device, mesh=mesh, in_specs=placed, out_specs=P("swath", "band"), check_vma=False
    )
```

```python
import functools

import jax
import jax.numpy as jnp
from jax import lax
from jax.experimental import pallas as pl
from jax.experimental.pallas import tpu as pltpu
from jax.sharding import PartitionSpec as P

NK = 8
KH = 16
IH = 4
BLK = 128
P_SIZE = 28
LANES = 128
EDGE = 32
PART = 32
GROUP = 4
REACH = 2 * KH + 1

epsilon = 1e-05
def pin(x):
    return pltpu.with_memory_space_constraint(x, pltpu.HBM)

F32 = jnp.float32
BF16 = jnp.bfloat16


def banded(offset, taps, shape):
    place = (
        lax.broadcasted_iota(jnp.int32, shape, 0)
        - lax.broadcasted_iota(jnp.int32, shape, 1)
        - offset
    )
    matrix = jnp.zeros(shape, F32)
    for tap, value in enumerate(taps):
        matrix = jnp.where(place == tap, value, matrix)
    return matrix


def banded_rows(offset, taps, shape):
    place = (
        lax.broadcasted_iota(jnp.int32, shape, 1)
        - lax.broadcasted_iota(jnp.int32, shape, 0)
        - offset
    )
    matrix = jnp.zeros(shape, F32)
    for tap, value in enumerate(taps):
        matrix = jnp.where(place == tap, value, matrix)
    return matrix


def kernel(
    n, height, width,
    weight_hbm, shift_hbm, phase_hbm, care_hbm,
    design_hbm, row_hbm, column_hbm, interp_hbm, image_hbm,
    filt, mean_ref, scale_ref,
    weight_ref, shift_ref, phase_ref, care_ref,
    design_ref, row_ref, column_ref, interp_ref,
    sendbuf, recv, image, row_mats, column_mats, taps, table, smooth, intensity,
    diff, stats_mine, stats_all,
    send_sem, recv_sem, stat_send, stat_recv, load_sem,
):
    me = lax.axis_index("band")
    rows = design_ref.shape[0]
    strip = width // n
    panels = strip // LANES
    wide = strip + LANES
    block_rows = GROUP * rows
    window = block_rows + 2 * KH
    steps = n // GROUP

    barrier = pltpu.get_barrier_semaphore()

    def greet(i, carry):
        peer = lax.rem(me + i, n)
        pl.semaphore_signal(
            barrier, inc=1, device_id={"band": peer}, device_id_type=pl.DeviceIdType.MESH
        )
        return carry

    lax.fori_loop(1, n, greet, 0)

    loads = [
        pltpu.make_async_copy(source, target, load_sem.at[i])
        for i, (source, target) in enumerate(
            [
                (design_hbm, design_ref),
                (row_hbm, row_ref),
                (column_hbm, column_ref),
                (interp_hbm, interp_ref),
                (weight_hbm, weight_ref),
                (shift_hbm, shift_ref),
                (phase_hbm, phase_ref),
                (care_hbm, care_ref),
                (image_hbm, image),
            ]
        )
    ]
    for load in loads:
        load.start()
    loads[0].wait()

    lane = lax.broadcasted_iota(jnp.int32, (rows, LANES), 1)
    low = lane < LANES // 2
    zero_panel = jnp.zeros((rows, LANES), BF16)
    for owner in range(n):
        start = owner * strip
        sendbuf[owner, :, :strip] = design_ref[:, start : start + strip]
        after = design_ref[:, start + strip : start + strip + LANES] if owner < n - 1 else zero_panel
        before = design_ref[:, start - LANES : start] if owner > 0 else zero_panel
        sendbuf[owner, :, strip:] = jnp.where(low, after, before)

    pl.semaphore_wait(barrier, n - 1)

    def copy_to(peer):
        return pltpu.make_async_remote_copy(
            src_ref=sendbuf.at[peer],
            dst_ref=recv.at[pl.ds(pl.multiple_of(KH + me * rows, rows), rows), :],
            send_sem=send_sem.at[peer],
            recv_sem=recv_sem.at[me],
            device_id={"band": peer},
            device_id_type=pl.DeviceIdType.MESH,
        )

    def copy_from(peer):
        return pltpu.make_async_remote_copy(
            src_ref=sendbuf.at[peer],
            dst_ref=recv.at[pl.ds(pl.multiple_of(KH + peer * rows, rows), rows), :],
            send_sem=send_sem.at[peer],
            recv_sem=recv_sem.at[peer],
            device_id={"band": peer},
            device_id_type=pl.DeviceIdType.MESH,
        )

    def send(i, carry):
        @pl.when(me + i < n)
        def _():
            copy_to(me + i).start()

        @pl.when(me - i >= 0)
        def _():
            copy_to(me - i).start()

        return carry

    lax.fori_loop(1, n, send, 0)

    recv[pl.ds(pl.multiple_of(KH + me * rows, rows), rows), :] = sendbuf[me]
    recv[:KH, :] = jnp.zeros((KH, wide), BF16)
    recv[KH + height :, :] = jnp.zeros((KH, wide), BF16)
    intensity[:EDGE, :] = jnp.zeros((EDGE, wide), BF16)
    intensity[EDGE + height :, :] = jnp.zeros((EDGE, wide), BF16)
    diff[:8, :] = jnp.zeros((8, strip), F32)
    diff[8 + height :, :] = jnp.zeros((8, strip), F32)

    for load in loads[1:-1]:
        load.wait()
    taps[:NK, :REACH] = row_ref[...].astype(F32)
    taps[NK:, :REACH] = column_ref[...].astype(F32)
    table[...] = interp_ref[...].astype(F32)
    phases = lax.broadcasted_iota(jnp.int32, table.shape, 1)

    def chosen(phase):
        row = jnp.sum(jnp.where(phases == phase, table[...], 0.0), axis=1, keepdims=True)
        return [row[t : t + 1] for t in range(2 * IH)]

    def build(k, carry):
        row_taps = [taps[pl.ds(k, 1), t : t + 1] for t in range(REACH)]
        row_mats[pl.ds(pl.multiple_of(k * block_rows, block_rows), block_rows), :] = banded_rows(
            0, row_taps, (block_rows, window)
        ).astype(BF16)
        column_taps = [taps[pl.ds(NK + k, 1), t : t + 1] for t in range(REACH)]
        column_mats[k] = banded(LANES - P_SIZE - KH, column_taps, (2 * LANES, LANES)).astype(BF16)
        return carry

    lax.fori_loop(0, NK, build, 0)

    rising = me < n // 2

    def arrived(place):
        band = jnp.where(rising, place, n - 1 - place)

        @pl.when(jnp.logical_and(place < n, band != me))
        def _():
            copy_from(band).wait_recv()

    first_column = me * strip - P_SIZE
    column = lax.broadcasted_iota(jnp.int32, (block_rows, LANES), 1)

    per_block = BLK // block_rows
    count = height // BLK
    part_rows = PART
    parts = BLK // part_rows

    def render(i, carry):
        for more in range(1, GROUP + 1):
            arrived(i * GROUP + more)
        group = jnp.where(rising, i, steps - 1 - i)
        start = pl.multiple_of(group * block_rows, block_rows)
        smooth[...] = jnp.dot(
            row_mats[...], recv[pl.ds(start, window), :], preferred_element_type=F32
        ).astype(BF16)
        total = jnp.zeros(((panels + 1) * block_rows, LANES), F32)
        for k in range(NK):
            own = smooth[k * block_rows : (k + 1) * block_rows, :]
            pieces = [jnp.concatenate([own[:, strip:], own[:, :LANES]], axis=1)]
            pieces += [own[:, (p - 1) * LANES : (p + 1) * LANES] for p in range(1, panels + 1)]
            field = jnp.dot(
                jnp.concatenate(pieces, axis=0), column_mats[k], preferred_element_type=F32
            )
            total = total + weight_ref[k] * field * field
        into = pl.multiple_of(EDGE + start, EDGE)
        for p in range(panels + 1):
            part = total[p * block_rows : (p + 1) * block_rows]
            if p in (0, panels):
                at = column + (first_column + p * LANES)
                part = jnp.where(jnp.logical_and(at >= 0, at < width), part, 0.0)
            intensity[pl.ds(into, block_rows), p * LANES : (p + 1) * LANES] = part.astype(BF16)

        @pl.when(jnp.logical_and(i >= per_block, lax.rem(i, per_block) == 0))
        def _():
            warp(i // per_block - 1)

        return carry

    def warp(place):
        b = jnp.where(rising, place, count - 1 - place)
        u = chosen(phase_ref[0, 0, b])
        v = chosen(phase_ref[1, 0, b])
        row_matrix = banded_rows(
            EDGE + 1 - IH + shift_ref[0, 0, b], u, (BLK, BLK + 2 * EDGE)
        ).astype(BF16)
        column_matrix = banded(
            P_SIZE + 1 - IH + shift_ref[1, 0, b], v, (2 * LANES, LANES)
        ).astype(BF16)
        start = pl.multiple_of(b * BLK, BLK)
        partial = jnp.dot(
            row_matrix, intensity[pl.ds(start, BLK + 2 * EDGE), :], preferred_element_type=F32
        ).astype(BF16)
        pieces = [partial[:, p * LANES : (p + 2) * LANES] for p in range(panels)]
        warped = jnp.dot(
            jnp.concatenate(pieces, axis=0), column_matrix, preferred_element_type=F32
        )
        care = care_ref[0, b].astype(F32)
        for p in range(panels):
            measured = image[pl.ds(start, BLK), p * LANES : (p + 1) * LANES].astype(F32)
            diff[pl.ds(pl.multiple_of(8 + start, 8), BLK), p * LANES : (p + 1) * LANES] = care * (
                measured - warped[p * BLK : (p + 1) * BLK]
            )

        first_part = place * parts - jnp.where(place > 0, 1, 0)
        last_part = (place + 1) * parts - jnp.where(place < count - 1, 1, 0)
        lax.fori_loop(first_part, last_part, stencil, 0)

    def stencil(place, carry):
        part = jnp.where(rising, place, count * parts - 1 - place)
        start = pl.multiple_of(part * part_rows, part_rows)
        around = diff[pl.ds(start, part_rows + 16), :]
        middle = around[8 : 8 + part_rows]
        value = middle + 0.5 * (around[7 : 7 + part_rows] + around[9 : 9 + part_rows])
        filt[pl.ds(start, part_rows), :] = value
        square = value * value
        first = stats_mine[:8, :]
        second = stats_mine[8:, :]
        for r in range(0, part_rows, 8):
            for p in range(panels):
                first = first + value[r : r + 8, p * LANES : (p + 1) * LANES]
                second = second + square[r : r + 8, p * LANES : (p + 1) * LANES]
        stats_mine[:8, :] = first
        stats_mine[8:, :] = second
        return carry

    loads[-1].wait()
    stats_mine[...] = jnp.zeros((16, LANES), F32)
    arrived(jnp.int32(0))
    lax.fori_loop(0, steps, render, 0)
    warp(jnp.int32(count - 1))

    def stat_to(peer):
        return pltpu.make_async_remote_copy(
            src_ref=stats_mine,
            dst_ref=stats_all.at[me],
            send_sem=stat_send.at[peer],
            recv_sem=stat_recv.at[me],
            device_id={"band": peer},
            device_id_type=pl.DeviceIdType.MESH,
        )

    def stat_from(peer):
        return pltpu.make_async_remote_copy(
            src_ref=stats_mine,
            dst_ref=stats_all.at[peer],
            send_sem=stat_send.at[peer],
            recv_sem=stat_recv.at[peer],
            device_id={"band": peer},
            device_id_type=pl.DeviceIdType.MESH,
        )

    def send_stats(i, carry):
        peer = lax.rem(me + n // 2 + i, n)

        @pl.when(peer != me)
        def _():
            stat_to(peer).start()

        return carry

    lax.fori_loop(0, n, send_stats, 0)
    stats_all[me] = stats_mine[...]

    def finish_sends(i, carry):
        peer = lax.rem(me + i, n)
        copy_to(peer).wait_send()
        return carry

    lax.fori_loop(1, n, finish_sends, 0)

    def take_stats(i, carry):
        peer = lax.rem(me + i, n)
        stat_from(peer).wait_recv()
        stat_to(peer).wait_send()
        return carry

    lax.fori_loop(1, n, take_stats, 0)

    sums = lax.fori_loop(
        0, n, lambda i, carry: carry + stats_all[i], jnp.zeros((16, LANES), F32)
    )
    cells = height * width
    mean = jnp.sum(jnp.sum(sums[:8], axis=1, keepdims=True), axis=0, keepdims=True) / cells
    power = jnp.sum(jnp.sum(sums[8:], axis=1, keepdims=True), axis=0, keepdims=True) / cells
    scale = lax.rsqrt(power - mean * mean + epsilon)
    mean_ref[...] = jnp.broadcast_to(mean, (1, strip))
    for b in range(count):
        scale_ref[b : b + 1, :] = jnp.broadcast_to(care_ref[0, b].astype(F32) * scale, (1, strip))


def on_device(
    design, row_taps, column_taps, kernel_weight, interp, block_shift, block_phase, care, image
):
    n = lax.axis_size("band")
    rows, width = design.shape
    height, strip = image.shape
    wide = strip + LANES
    block_rows = GROUP * rows
    window = block_rows + 2 * KH
    count = height // BLK
    hbm = pl.BlockSpec(memory_space=pltpu.HBM)
    vmem = pl.BlockSpec(memory_space=pltpu.VMEM)
    filtered, mean, scale = pl.pallas_call(
        functools.partial(kernel, n, height, width),
        out_shape=(
            jax.ShapeDtypeStruct((height, strip), F32),
            jax.ShapeDtypeStruct((1, strip), F32),
            jax.ShapeDtypeStruct((count, strip), F32),
        ),
        in_specs=[hbm] * 9,
        out_specs=(vmem, vmem, vmem),
        scratch_shapes=[
            pltpu.SMEM((NK,), F32),
            pltpu.SMEM((2, 1, count), jnp.int32),
            pltpu.SMEM((2, 1, count), jnp.int32),
            pltpu.SMEM((1, count), jnp.int32),
            pltpu.VMEM((rows, width), BF16),
            pltpu.VMEM(row_taps.shape, BF16),
            pltpu.VMEM(column_taps.shape, BF16),
            pltpu.VMEM(interp.shape[::-1], BF16),
            pltpu.VMEM((n, rows, wide), BF16),
            pltpu.VMEM((height + 2 * KH, wide), BF16),
            pltpu.VMEM((height, strip), BF16),
            pltpu.VMEM((NK * block_rows, window), BF16),
            pltpu.VMEM((NK, 2 * LANES, LANES), BF16),
            pltpu.VMEM((2 * NK, LANES), F32),
            pltpu.VMEM(interp.shape[::-1], F32),
            pltpu.VMEM((NK * block_rows, wide), BF16),
            pltpu.VMEM((height + 2 * EDGE, wide), BF16),
            pltpu.VMEM((height + 16, strip), F32),
            pltpu.VMEM((16, LANES), F32),
            pltpu.VMEM((n, 16, LANES), F32),
            pltpu.SemaphoreType.DMA((n,)),
            pltpu.SemaphoreType.DMA((n,)),
            pltpu.SemaphoreType.DMA((n,)),
            pltpu.SemaphoreType.DMA((n,)),
            pltpu.SemaphoreType.DMA((9,)),
        ],
        compiler_params=pltpu.CompilerParams(
            collective_id=0, has_side_effects=True, vmem_limit_bytes=32 * 1024 * 1024
        ),
    )(
        pin(kernel_weight),
        pin(jnp.transpose(block_shift, (0, 2, 1))),
        pin(jnp.transpose(block_phase, (0, 2, 1))),
        pin(care.T),
        pin(design),
        pin(row_taps),
        pin(column_taps),
        pin(interp.T),
        pin(image),
    )
    blocks = filtered.reshape(count, BLK, strip)
    out = (blocks - mean[:, None]) * scale[:, None]
    return out.reshape(height, strip).astype(BF16)


def solution(mesh):
    placed = (
        P(("swath", "band"), None),
        P(),
        P(),
        P(),
        P(),
        P(None, "swath", "band"),
        P(None, "swath", "band"),
        P("swath", "band"),
        P("swath", "band"),
    )
    return jax.shard_map(
        on_device, mesh=mesh, in_specs=placed, out_specs=P("swath", "band"), check_vma=False
    )
```

```python
import functools

import jax
import jax.numpy as jnp
from jax import lax
from jax.experimental import pallas as pl
from jax.experimental.pallas import tpu as pltpu
from jax.sharding import PartitionSpec as P

NK = 8
KH = 16
IH = 4
BLK = 128
P_SIZE = 28
LANES = 128
EDGE = 32
PART = 32
GROUP = 4
REACH = 2 * KH + 1

epsilon = 1e-05
def pin(x):
    return pltpu.with_memory_space_constraint(x, pltpu.HBM)

F32 = jnp.float32
BF16 = jnp.bfloat16


def banded(offset, taps, shape):
    place = (
        lax.broadcasted_iota(jnp.int32, shape, 0)
        - lax.broadcasted_iota(jnp.int32, shape, 1)
        - offset
    )
    matrix = jnp.zeros(shape, F32)
    for tap, value in enumerate(taps):
        matrix = jnp.where(place == tap, value, matrix)
    return matrix


def banded_rows(offset, taps, shape):
    place = (
        lax.broadcasted_iota(jnp.int32, shape, 1)
        - lax.broadcasted_iota(jnp.int32, shape, 0)
        - offset
    )
    matrix = jnp.zeros(shape, F32)
    for tap, value in enumerate(taps):
        matrix = jnp.where(place == tap, value, matrix)
    return matrix


def kernel(
    n, height, width,
    weight_hbm, shift_hbm, phase_hbm, care_hbm,
    design_hbm, row_hbm, column_hbm, interp_hbm, image_hbm,
    filt, mean_ref, scale_ref,
    weight_ref, shift_ref, phase_ref, care_ref,
    design_ref, row_ref, column_ref, interp_ref,
    sendbuf, recv, image, row_mats, column_mats, taps, table, smooth, intensity,
    diff, partial_sums, stats_mine, stats_all,
    send_sem, recv_sem, stat_send, stat_recv, load_sem,
):
    me = lax.axis_index("band")
    rows = design_ref.shape[0]
    strip = width // n
    panels = strip // LANES
    wide = strip + LANES
    block_rows = GROUP * rows
    window = block_rows + 2 * KH
    steps = n // GROUP

    barrier = pltpu.get_barrier_semaphore()

    def greet(i, carry):
        peer = lax.rem(me + i, n)
        pl.semaphore_signal(
            barrier, inc=1, device_id={"band": peer}, device_id_type=pl.DeviceIdType.MESH
        )
        return carry

    lax.fori_loop(1, n, greet, 0)

    loads = [
        pltpu.make_async_copy(source, target, load_sem.at[i])
        for i, (source, target) in enumerate(
            [
                (design_hbm, design_ref),
                (row_hbm, row_ref),
                (column_hbm, column_ref),
                (interp_hbm, interp_ref),
                (weight_hbm, weight_ref),
                (shift_hbm, shift_ref),
                (phase_hbm, phase_ref),
                (care_hbm, care_ref),
                (image_hbm, image),
            ]
        )
    ]
    for load in loads:
        load.start()
    loads[0].wait()

    lane = lax.broadcasted_iota(jnp.int32, (rows, LANES), 1)
    low = lane < LANES // 2
    zero_panel = jnp.zeros((rows, LANES), BF16)
    for owner in range(n):
        start = owner * strip
        sendbuf[owner, :, :strip] = design_ref[:, start : start + strip]
        after = design_ref[:, start + strip : start + strip + LANES] if owner < n - 1 else zero_panel
        before = design_ref[:, start - LANES : start] if owner > 0 else zero_panel
        sendbuf[owner, :, strip:] = jnp.where(low, after, before)

    pl.semaphore_wait(barrier, n - 1)

    def copy_to(peer):
        return pltpu.make_async_remote_copy(
            src_ref=sendbuf.at[peer],
            dst_ref=recv.at[pl.ds(pl.multiple_of(KH + me * rows, rows), rows), :],
            send_sem=send_sem.at[peer],
            recv_sem=recv_sem.at[me],
            device_id={"band": peer},
            device_id_type=pl.DeviceIdType.MESH,
        )

    def copy_from(peer):
        return pltpu.make_async_remote_copy(
            src_ref=sendbuf.at[peer],
            dst_ref=recv.at[pl.ds(pl.multiple_of(KH + peer * rows, rows), rows), :],
            send_sem=send_sem.at[peer],
            recv_sem=recv_sem.at[peer],
            device_id={"band": peer},
            device_id_type=pl.DeviceIdType.MESH,
        )

    def send(i, carry):
        @pl.when(me + i < n)
        def _():
            copy_to(me + i).start()

        @pl.when(me - i >= 0)
        def _():
            copy_to(me - i).start()

        return carry

    lax.fori_loop(1, n, send, 0)

    recv[pl.ds(pl.multiple_of(KH + me * rows, rows), rows), :] = sendbuf[me]
    recv[:KH, :] = jnp.zeros((KH, wide), BF16)
    recv[KH + height :, :] = jnp.zeros((KH, wide), BF16)
    intensity[:EDGE, :] = jnp.zeros((EDGE, wide), BF16)
    intensity[EDGE + height :, :] = jnp.zeros((EDGE, wide), BF16)
    diff[:8, :] = jnp.zeros((8, strip), F32)
    diff[8 + height :, :] = jnp.zeros((8, strip), F32)

    for load in loads[1:-1]:
        load.wait()
    taps[:NK, :REACH] = row_ref[...].astype(F32)
    taps[NK:, :REACH] = column_ref[...].astype(F32)
    table[...] = interp_ref[...].astype(F32)
    phases = lax.broadcasted_iota(jnp.int32, table.shape, 1)

    def chosen(phase):
        row = jnp.sum(jnp.where(phases == phase, table[...], 0.0), axis=1, keepdims=True)
        return [row[t : t + 1] for t in range(2 * IH)]

    def build(k, carry):
        row_taps = [taps[pl.ds(k, 1), t : t + 1] for t in range(REACH)]
        row_mats[pl.ds(pl.multiple_of(k * block_rows, block_rows), block_rows), :] = banded_rows(
            0, row_taps, (block_rows, window)
        ).astype(BF16)
        column_taps = [taps[pl.ds(NK + k, 1), t : t + 1] for t in range(REACH)]
        column_mats[k] = banded(LANES - P_SIZE - KH, column_taps, (2 * LANES, LANES)).astype(BF16)
        return carry

    lax.fori_loop(0, NK, build, 0)

    rising = me < n // 2

    def arrived(place):
        band = jnp.where(rising, place, n - 1 - place)

        @pl.when(jnp.logical_and(place < n, band != me))
        def _():
            copy_from(band).wait_recv()

    first_column = me * strip - P_SIZE
    column = lax.broadcasted_iota(jnp.int32, (block_rows, LANES), 1)

    per_block = BLK // block_rows
    count = height // BLK
    part_rows = PART
    parts = BLK // part_rows

    def render(i, carry):
        for more in range(1, GROUP + 1):
            arrived(i * GROUP + more)
        group = jnp.where(rising, i, steps - 1 - i)
        start = pl.multiple_of(group * block_rows, block_rows)
        smooth[...] = jnp.dot(
            row_mats[...], recv[pl.ds(start, window), :], preferred_element_type=F32
        ).astype(BF16)
        total = jnp.zeros(((panels + 1) * block_rows, LANES), F32)
        for k in range(NK):
            own = smooth[k * block_rows : (k + 1) * block_rows, :]
            pieces = [jnp.concatenate([own[:, strip:], own[:, :LANES]], axis=1)]
            pieces += [own[:, (p - 1) * LANES : (p + 1) * LANES] for p in range(1, panels + 1)]
            field = jnp.dot(
                jnp.concatenate(pieces, axis=0), column_mats[k], preferred_element_type=F32
            )
            total = total + weight_ref[k] * field * field
        into = pl.multiple_of(EDGE + start, EDGE)
        for p in range(panels + 1):
            part = total[p * block_rows : (p + 1) * block_rows]
            if p in (0, panels):
                at = column + (first_column + p * LANES)
                part = jnp.where(jnp.logical_and(at >= 0, at < width), part, 0.0)
            intensity[pl.ds(into, block_rows), p * LANES : (p + 1) * LANES] = part.astype(BF16)

        @pl.when(jnp.logical_and(i >= per_block, lax.rem(i, per_block) == 0))
        def _():
            warp(i // per_block - 1)

        return carry

    def warp(place):
        b = jnp.where(rising, place, count - 1 - place)
        u = chosen(phase_ref[0, 0, b])
        v = chosen(phase_ref[1, 0, b])
        row_matrix = banded_rows(
            EDGE + 1 - IH + shift_ref[0, 0, b], u, (BLK, BLK + 2 * EDGE)
        ).astype(BF16)
        column_matrix = banded(
            P_SIZE + 1 - IH + shift_ref[1, 0, b], v, (2 * LANES, LANES)
        ).astype(BF16)
        start = pl.multiple_of(b * BLK, BLK)
        partial = jnp.dot(
            row_matrix, intensity[pl.ds(start, BLK + 2 * EDGE), :], preferred_element_type=F32
        ).astype(BF16)
        pieces = [partial[:, p * LANES : (p + 2) * LANES] for p in range(panels)]
        warped = jnp.dot(
            jnp.concatenate(pieces, axis=0), column_matrix, preferred_element_type=F32
        )
        care = care_ref[0, b].astype(F32)
        for p in range(panels):
            measured = image[pl.ds(start, BLK), p * LANES : (p + 1) * LANES].astype(F32)
            diff[pl.ds(pl.multiple_of(8 + start, 8), BLK), p * LANES : (p + 1) * LANES] = care * (
                measured - warped[p * BLK : (p + 1) * BLK]
            )

        first_part = place * parts - jnp.where(place > 0, 1, 0)
        last_part = (place + 1) * parts - jnp.where(place < count - 1, 1, 0)
        lax.fori_loop(first_part, last_part, stencil, 0)

    def stencil(place, carry):
        part = jnp.where(rising, place, count * parts - 1 - place)
        start = pl.multiple_of(part * part_rows, part_rows)
        around = diff[pl.ds(start, part_rows + 16), :]
        middle = around[8 : 8 + part_rows]
        value = middle + 0.5 * (around[7 : 7 + part_rows] + around[9 : 9 + part_rows])
        filt[pl.ds(start, part_rows), :] = value
        square = value * value
        first = partial_sums[:8, :]
        second = partial_sums[8:, :]
        for r in range(0, part_rows, 8):
            for p in range(panels):
                first = first + value[r : r + 8, p * LANES : (p + 1) * LANES]
                second = second + square[r : r + 8, p * LANES : (p + 1) * LANES]
        partial_sums[:8, :] = first
        partial_sums[8:, :] = second
        return carry

    loads[-1].wait()
    partial_sums[...] = jnp.zeros((16, LANES), F32)
    arrived(jnp.int32(0))
    lax.fori_loop(0, steps, render, 0)
    warp(jnp.int32(count - 1))
    stats_mine[0:1, :] = jnp.sum(partial_sums[:8, :], axis=0, keepdims=True)
    stats_mine[1:2, :] = jnp.sum(partial_sums[8:, :], axis=0, keepdims=True)

    def stat_to(peer):
        return pltpu.make_async_remote_copy(
            src_ref=stats_mine,
            dst_ref=stats_all.at[me],
            send_sem=stat_send.at[peer],
            recv_sem=stat_recv.at[me],
            device_id={"band": peer},
            device_id_type=pl.DeviceIdType.MESH,
        )

    def stat_from(peer):
        return pltpu.make_async_remote_copy(
            src_ref=stats_mine,
            dst_ref=stats_all.at[peer],
            send_sem=stat_send.at[peer],
            recv_sem=stat_recv.at[peer],
            device_id={"band": peer},
            device_id_type=pl.DeviceIdType.MESH,
        )

    def send_stats(i, carry):
        peer = lax.rem(me + n // 2 + i, n)

        @pl.when(peer != me)
        def _():
            stat_to(peer).start()

        return carry

    lax.fori_loop(0, n, send_stats, 0)
    stats_all[me] = stats_mine[...]

    def finish_sends(i, carry):
        peer = lax.rem(me + i, n)
        copy_to(peer).wait_send()
        return carry

    lax.fori_loop(1, n, finish_sends, 0)

    def take_stats(i, carry):
        peer = lax.rem(me + i, n)
        stat_from(peer).wait_recv()
        stat_to(peer).wait_send()
        return carry

    lax.fori_loop(1, n, take_stats, 0)

    sums = lax.fori_loop(
        0, n, lambda i, carry: carry + stats_all[i], jnp.zeros((2, LANES), F32)
    )
    cells = height * width
    mean = jnp.sum(sums[0:1], axis=1, keepdims=True) / cells
    power = jnp.sum(sums[1:2], axis=1, keepdims=True) / cells
    scale = lax.rsqrt(power - mean * mean + epsilon)
    mean_ref[...] = jnp.broadcast_to(mean, (1, strip))
    for b in range(count):
        scale_ref[b : b + 1, :] = jnp.broadcast_to(care_ref[0, b].astype(F32) * scale, (1, strip))


def on_device(
    design, row_taps, column_taps, kernel_weight, interp, block_shift, block_phase, care, image
):
    n = lax.axis_size("band")
    rows, width = design.shape
    height, strip = image.shape
    wide = strip + LANES
    block_rows = GROUP * rows
    window = block_rows + 2 * KH
    count = height // BLK
    hbm = pl.BlockSpec(memory_space=pltpu.HBM)
    vmem = pl.BlockSpec(memory_space=pltpu.VMEM)
    filtered, mean, scale = pl.pallas_call(
        functools.partial(kernel, n, height, width),
        out_shape=(
            jax.ShapeDtypeStruct((height, strip), F32),
            jax.ShapeDtypeStruct((1, strip), F32),
            jax.ShapeDtypeStruct((count, strip), F32),
        ),
        in_specs=[hbm] * 9,
        out_specs=(vmem, vmem, vmem),
        scratch_shapes=[
            pltpu.SMEM((NK,), F32),
            pltpu.SMEM((2, 1, count), jnp.int32),
            pltpu.SMEM((2, 1, count), jnp.int32),
            pltpu.SMEM((1, count), jnp.int32),
            pltpu.VMEM((rows, width), BF16),
            pltpu.VMEM(row_taps.shape, BF16),
            pltpu.VMEM(column_taps.shape, BF16),
            pltpu.VMEM(interp.shape[::-1], BF16),
            pltpu.VMEM((n, rows, wide), BF16),
            pltpu.VMEM((height + 2 * KH, wide), BF16),
            pltpu.VMEM((height, strip), BF16),
            pltpu.VMEM((NK * block_rows, window), BF16),
            pltpu.VMEM((NK, 2 * LANES, LANES), BF16),
            pltpu.VMEM((2 * NK, LANES), F32),
            pltpu.VMEM(interp.shape[::-1], F32),
            pltpu.VMEM((NK * block_rows, wide), BF16),
            pltpu.VMEM((height + 2 * EDGE, wide), BF16),
            pltpu.VMEM((height + 16, strip), F32),
            pltpu.VMEM((16, LANES), F32),
            pltpu.VMEM((2, LANES), F32),
            pltpu.VMEM((n, 2, LANES), F32),
            pltpu.SemaphoreType.DMA((n,)),
            pltpu.SemaphoreType.DMA((n,)),
            pltpu.SemaphoreType.DMA((n,)),
            pltpu.SemaphoreType.DMA((n,)),
            pltpu.SemaphoreType.DMA((9,)),
        ],
        compiler_params=pltpu.CompilerParams(
            collective_id=0, has_side_effects=True, vmem_limit_bytes=32 * 1024 * 1024
        ),
    )(
        pin(kernel_weight),
        pin(jnp.transpose(block_shift, (0, 2, 1))),
        pin(jnp.transpose(block_phase, (0, 2, 1))),
        pin(care.T),
        pin(design),
        pin(row_taps),
        pin(column_taps),
        pin(interp.T),
        pin(image),
    )
    blocks = filtered.reshape(count, BLK, strip)
    out = (blocks - mean[:, None]) * scale[:, None]
    return out.reshape(height, strip).astype(BF16)


def solution(mesh):
    placed = (
        P(("swath", "band"), None),
        P(),
        P(),
        P(),
        P(),
        P(None, "swath", "band"),
        P(None, "swath", "band"),
        P("swath", "band"),
        P("swath", "band"),
    )
    return jax.shard_map(
        on_device, mesh=mesh, in_specs=placed, out_specs=P("swath", "band"), check_vma=False
    )
```
